32 devices in a mesh: dp: 1 (over z), tp: 4 (over y), pp: 8 (over x, core).
Axes of the slice: x: 4, y: 4, z: 1, core: 2. Of those that a mesh axis runs over, the one named last changes fastest.
The devices are a block of a 4x4x8 slice.
Arguments:
- x: bfloat16 [8, 256, 1024], P('dp')
- target: bfloat16 [8, 256, 1024], P('dp')
- w1: bfloat16 [8, 2, 1024, 4096], P(('dp', 'pp'), None, None, 'tp')
- w2: bfloat16 [8, 2, 4096, 1024], P(('dp', 'pp'), None, 'tp')
Outputs:
- output 1: float32 [8, 2, 1024, 4096], P(('dp', 'pp'), None, None, 'tp')
- output 2: float32 [8, 2, 4096, 1024], P(('dp', 'pp'), None, 'tp')
- output 3: float32 [1], P('dp')
All inputs are finite; a program needn't handle non-finite values.
Results may differ from the reference program's by a relative error of at most 0.0182704.
Values are sent between devices in bfloat16 or wider.
A program may use at most 768 MiB of HBM per device.

```python
import math
import jax
import jax.numpy as jnp
from jax import lax

STAGES = 8
NL = 2
M = 8
B = 256
D = 1024
FF = 4096

LAYERS = STAGES * NL
GC = math.sqrt(2.0 / math.pi)


def gelu(v):
    return 0.5 * v * (1.0 + jnp.tanh(GC * (v + 0.044715 * v * v * v)))


def gelu_grad(v):
    t = jnp.tanh(GC * (v + 0.044715 * v * v * v))
    return 0.5 * (1.0 + t) + 0.5 * v * (1.0 - t * t) * GC * (1.0 + 0.134145 * v * v)


def setup_inputs(seed: int = 0, part: int = 0) -> dict:
    key = jax.random.fold_in(jax.random.key(seed), part)
    kx, ky, k1, k2 = jax.random.split(key, 4)
    x = jax.random.normal(kx, (M, B, D), jnp.float32)
    target = jax.random.normal(ky, (M, B, D), jnp.float32)
    w1 = jax.random.normal(k1, (STAGES, NL, D, FF), jnp.float32) * D ** -0.5
    w2 = jax.random.normal(k2, (STAGES, NL, FF, D), jnp.float32) * (FF * LAYERS) ** -0.5
    return {'x': x.astype(jnp.bfloat16), 'target': target.astype(jnp.bfloat16),
            'w1': w1.astype(jnp.bfloat16), 'w2': w2.astype(jnp.bfloat16)}


def layer_fwd(h, w1, w2):
    u = jnp.dot(h, w1, preferred_element_type=jnp.float32).astype(jnp.bfloat16)
    a = gelu(u.astype(jnp.float32)).astype(jnp.bfloat16)
    z = jnp.dot(a, w2, preferred_element_type=jnp.float32)
    return (h.astype(jnp.float32) + z).astype(jnp.bfloat16), u


def layer_bwd(h, u, dh, w1, w2):
    uf = u.astype(jnp.float32)
    a = gelu(uf).astype(jnp.bfloat16)
    da = jnp.dot(dh, w2.T, preferred_element_type=jnp.float32)
    g = (gelu_grad(uf) * da).astype(jnp.bfloat16)
    dx = (dh.astype(jnp.float32) + jnp.dot(g, w1.T, preferred_element_type=jnp.float32)).astype(jnp.bfloat16)
    return dx, jnp.dot(h.T, g, preferred_element_type=jnp.float32), jnp.dot(a.T, dh, preferred_element_type=jnp.float32)


def reference(x, target, w1, w2):
    w1s = w1.reshape(LAYERS, D, FF)
    w2s = w2.reshape(LAYERS, FF, D)
    scale = (M * B) ** -0.5

    def micro(carry, xt):
        acc1, acc2, loss = carry
        xm, tm = xt

        def fstep(h, w):
            hn, u = layer_fwd(h, w[0], w[1])
            return hn, (h, u)

        out, (hs, us) = lax.scan(fstep, xm, (w1s, w2s))
        diff = out.astype(jnp.float32) - tm.astype(jnp.float32)
        loss = loss + 0.5 * jnp.sum(diff * diff) / (M * B * D)
        dy = (diff * scale).astype(jnp.bfloat16)

        def bstep(dh, z):
            h, u, a1, a2, wa, wb = z
            dx, d1, d2 = layer_bwd(h, u, dh, wa, wb)
            return dx, (a1 + d1, a2 + d2)

        _, (acc1, acc2) = lax.scan(bstep, dy, (hs, us, acc1, acc2, w1s, w2s), reverse=True)
        return (acc1, acc2, loss), None

    init = (jnp.zeros((LAYERS, D, FF), jnp.float32), jnp.zeros((LAYERS, FF, D), jnp.float32),
            jnp.zeros((), jnp.float32))
    (acc1, acc2, loss), _ = lax.scan(micro, init, (x, target))
    return acc1.reshape(STAGES, NL, D, FF), acc2.reshape(STAGES, NL, FF, D), loss.reshape(1)
```

```python
import functools
import math
import jax
import jax.numpy as jnp
from jax import lax
from jax.experimental import pallas as pl
from jax.experimental.pallas import tpu as pltpu
from jax.sharding import PartitionSpec as P

GC = math.sqrt(2.0 / math.pi)
BF = jnp.bfloat16
F32 = jnp.float32
MESH = pl.DeviceIdType.MESH
CHUNK = 128


def gelu_parts(v):
    return jnp.tanh(GC * (v + 0.044715 * v * v * v))


def dot(a, b):
    return jnp.dot(a, b, preferred_element_type=F32)


def dot_t(a, b):
    return lax.dot_general(a, b, (((1,), (1,)), ((), ())), preferred_element_type=F32)


def dot_l(a, b):
    return lax.dot_general(a, b, (((0,), (0,)), ((), ())), preferred_element_type=F32)


def kernel(ntp, npp, scale, x_hbm, t_hbm, w1_hbm, w2_hbm, g1_hbm, g2_hbm, loss_ref,
           w1, w2, xs, ds, u, g, hs, hb, zs, zr, zsb, zrb, a_buf, zown, lacc, lbuf,
           in_sem, ws_sem, wr_sem, gs_sem, gr_sem, fl_s, fl_r, fa_s, fa_r, fz_s, fz_r,
           bl_s, bl_r, ba_s, ba_r, bz_s, bz_r, ls_sem, lr_sem):
    ntok, hd = hs.shape
    nl, d, fl = w1_hbm.shape
    ct = CHUNK
    nc = ntok // ct
    y = lax.axis_index('tp')
    pp = lax.axis_index('pp')
    c = lax.rem(pp, 2)
    o = 1 - c
    xc = lax.div(pp, 2)
    odd = lax.rem(xc, 2)
    r = y + odd * (ntp - 1 - 2 * y)
    k = xc * ntp + r
    nk = ntp * npp // 2
    first = k == 0
    last = k == nk - 1
    step = 1 - 2 * odd
    fwd_end = jnp.where(r == ntp - 1, 1, 0)
    bwd_end = jnp.where(r == 0, 1, 0)
    nxt = {'tp': y + step * (1 - fwd_end), 'pp': jnp.where(last, c, pp + 2 * fwd_end)}
    nxt['tp'] = jnp.where(last, 0, nxt['tp'])
    prv = {'tp': y - step * (1 - bwd_end), 'pp': jnp.where(first, npp - 2 + c, pp - 2 * bwd_end)}
    row_end = (ntp - 1) * (1 - lax.rem(npp // 2 - 1, 2))
    prv['tp'] = jnp.where(first, row_end, prv['tp'])
    mate = {'tp': y, 'pp': 2 * xc + o}

    barrier = pltpu.get_barrier_semaphore()
    for j in range(1, 2 * ntp):
        idx = lax.rem(y * 2 + c + j, 2 * ntp)
        pl.semaphore_signal(barrier, inc=1, device_id={'tp': lax.div(idx, 2), 'pp': 2 * xc + lax.rem(idx, 2)},
                            device_id_type=MESH)
    pl.semaphore_signal(barrier, inc=1, device_id=nxt, device_id_type=MESH)
    pl.semaphore_signal(barrier, inc=1, device_id=prv, device_id_type=MESH)
    pl.semaphore_wait(barrier, 2 * ntp + 1)

    def rcopy(src, dst, ss, rs, dev):
        return pltpu.make_async_remote_copy(src_ref=src, dst_ref=dst, send_sem=ss, recv_sem=rs,
                                            device_id=dev, device_id_type=MESH)

    for i in range(nl):
        rr = nl * c + i
        row = rr + odd * (ntp - 1 - 2 * rr)
        dst = {'tp': row, 'pp': 2 * xc + lax.div(y, 2)}
        same = (row == y) & (lax.div(y, 2) == c)
        b = lax.rem(y, 2)
        for n, (src, buf) in enumerate(((w1_hbm, w1), (w2_hbm, w2))):
            @pl.when(same)
            def _():
                pltpu.make_async_copy(src.at[i], buf.at[b], wr_sem.at[n, b]).start()

            @pl.when(jnp.logical_not(same))
            def _():
                rcopy(src.at[i], buf.at[b], ws_sem.at[n, i], wr_sem.at[n, b], dst).start()

    @pl.when(first)
    def _():
        for h in range(2):
            pltpu.make_async_copy(x_hbm.at[:, pl.ds(h * hd, hd)], xs.at[h], in_sem.at[h]).start()

    @pl.when(last)
    def _():
        pltpu.make_async_copy(t_hbm.at[:, pl.ds(pl.multiple_of(c * hd, hd), hd)], hs, in_sem.at[2]).start()

    lacc[...] = jnp.zeros_like(lacc)

    def wwait(n, b):
        src, buf = ((w1_hbm, w1), (w2_hbm, w2))[n]
        rcopy(src.at[0], buf.at[b], ws_sem.at[n, 0], wr_sem.at[n, b], mate).wait_recv()

    for n in range(2):
        for b in range(2):
            wwait(n, b)

    @pl.when(first)
    def _():
        for h in range(2):
            pltpu.make_async_copy(x_hbm.at[:, pl.ds(h * hd, hd)], xs.at[h], in_sem.at[h]).wait()

    @pl.when(last)
    def _():
        pltpu.make_async_copy(t_hbm.at[:, pl.ds(pl.multiple_of(c * hd, hd), hd)], hs, in_sem.at[2]).wait()

    def rows(m):
        return pl.ds(pl.multiple_of(m * ct, ct), ct)

    def cp_link(buf, store, m, ss, rs, dev):
        return rcopy(buf.at[rows(m)], store.at[c, rows(m)], ss.at[m], rs.at[m], dev)

    def cp_ag(store, half, m, ss, rs):
        return rcopy(store.at[half, rows(m)], store.at[half, rows(m)], ss.at[m], rs.at[m], mate)

    def cp_rs(src, dst, m, ss, rs):
        return rcopy(src.at[rows(m)], dst.at[rows(m)], ss.at[m], rs.at[m], mate)

    def get_f(m):
        cp_link(hs, xs, m, fl_s, fl_r, nxt).wait_recv()
        cp_ag(xs, c, m, fa_s, fa_r).start()

    @pl.when(jnp.logical_not(first))
    def _():
        get_f(0)

    half_o = pl.ds(pl.multiple_of(o * hd, hd), hd)
    half_c = pl.ds(pl.multiple_of(c * hd, hd), hd)
    tn = fl // 2

    def fwd(m, _):
        @pl.when(jnp.logical_not(first))
        def _():
            cp_ag(xs, o, m, fa_s, fa_r).wait_recv()

        rw = rows(m)
        for q in range(2):
            for t in range(fl // tn):
                s = pl.ds(t * tn, tn)
                v = (dot(xs[0, rw, :], w1[q, :hd, s]) + dot(xs[1, rw, :], w1[q, hd:, s])).astype(BF)
                u[q, rw, s] = v
                v = v.astype(F32)
                a_buf[q, :, s] = (0.5 * v * (1.0 + gelu_parts(v))).astype(BF)
        zs[rw, :] = (dot(a_buf[0], w2[0, :, half_o]) + dot(a_buf[1], w2[1, :, half_o])).astype(BF)
        cp_rs(zs, zr, m, fz_s, fz_r).start()
        zown[...] = (xs[c, rw, :].astype(F32)
                     + (dot(a_buf[0], w2[0, :, half_c]) + dot(a_buf[1], w2[1, :, half_c])))

        @pl.when(jnp.logical_not(first) & (m + 1 < nc))
        def _():
            get_f(m + 1)

        cp_rs(zs, zr, m, fz_s, fz_r).wait_recv()
        out = (zown[...] + zr[rw, :].astype(F32)).astype(BF)

        @pl.when(jnp.logical_not(last))
        def _():
            hs[rw, :] = out
            cp_link(hs, xs, m, fl_s, fl_r, nxt).start()

        @pl.when(last)
        def _():
            diff = out.astype(F32) - hs[rw, :].astype(F32)
            ds[c, rw, :] = (diff * scale).astype(BF)
            sq = jnp.sum((diff * diff).reshape(ct // 8, 8, hd), axis=0)
            tot = lacc[...]
            for j in range(hd // 128):
                tot = tot + sq[:, j * 128:(j + 1) * 128]
            lacc[...] = tot

        return 0

    lax.fori_loop(0, nc, fwd, 0)

    def get_b(m):
        @pl.when(jnp.logical_not(last))
        def _():
            cp_link(hb, ds, m, bl_s, bl_r, prv).wait_recv()

        cp_ag(ds, c, m, ba_s, ba_r).start()

    get_b(0)

    def bwd(m, _):
        cp_ag(ds, o, m, ba_s, ba_r).wait_recv()
        rw = rows(m)
        for q in range(2):
            for t in range(fl // tn):
                s = pl.ds(t * tn, tn)
                da = dot_t(ds[0, rw, :], w2[q, s, :hd]) + dot_t(ds[1, rw, :], w2[q, s, hd:])
                v = u[q, rw, s].astype(F32)
                th = gelu_parts(v)
                gp = 0.5 * (1.0 + th) + 0.5 * v * (1.0 - th * th) * GC * (1.0 + 0.134145 * v * v)
                g[q, rw, s] = (gp * da).astype(BF)
                u[q, rw, s] = (0.5 * v * (1.0 + th)).astype(BF)

        @pl.when(jnp.logical_not(first))
        def _():
            zsb[rw, :] = (dot_t(g[0, rw, :], w1[0, half_o, :]) + dot_t(g[1, rw, :], w1[1, half_o, :])).astype(BF)
            cp_rs(zsb, zrb, m, bz_s, bz_r).start()
            zown[...] = (ds[c, rw, :].astype(F32)
                         + (dot_t(g[0, rw, :], w1[0, half_c, :]) + dot_t(g[1, rw, :], w1[1, half_c, :])))

        @pl.when(m + 1 < nc)
        def _():
            get_b(m + 1)

        @pl.when(jnp.logical_not(first))
        def _():
            cp_rs(zsb, zrb, m, bz_s, bz_r).wait_recv()
            hb[rw, :] = (zown[...] + zrb[rw, :].astype(F32)).astype(BF)
            cp_link(hb, ds, m, bl_s, bl_r, prv).start()

        return 0

    lax.fori_loop(0, nc, bwd, 0)

    @pl.when(last)
    def _():
        lbuf[0] = lacc[...]
        cp = rcopy(lbuf.at[0], lbuf.at[1], ls_sem.at[0], lr_sem.at[0], mate)
        cp.start()
        cp.wait()
        lbuf[2] = lbuf[0] + lbuf[1]

    @pl.when(jnp.logical_not(last))
    def _():
        rcopy(lbuf.at[2], lbuf.at[2], ls_sem.at[1], lr_sem.at[1], prv).wait_recv()

    @pl.when(jnp.logical_not(first))
    def _():
        rcopy(lbuf.at[2], lbuf.at[2], ls_sem.at[1], lr_sem.at[1], prv).start()

    i_own = lax.rem(r, nl)
    src_core = lax.div(r, nl)

    def send_g(n, b, wait):
        buf, out = ((w1, g1_hbm), (w2, g2_hbm))[n]
        row = 2 * c + b
        same = (row == y) & (src_core == c)
        dst = {'tp': row, 'pp': 2 * xc + src_core}

        if not wait:
            @pl.when(same)
            def _():
                pltpu.make_async_copy(buf.at[b], out.at[i_own], gr_sem.at[n, i_own]).start()

        @pl.when(jnp.logical_not(same))
        def _():
            cp = rcopy(buf.at[b], out.at[i_own], gs_sem.at[n, b], gr_sem.at[n, i_own], dst)
            if wait:
                cp.wait_send()
            else:
                cp.start()

    tm = 256

    for b in range(2):
        def dw2(t, _):
            s = pl.ds(pl.multiple_of(t * tm, tm), tm)
            for h in range(2):
                w2[b, s, h * hd:(h + 1) * hd] = dot_l(u[b, :, s], ds[h]).astype(BF)
            return 0

        lax.fori_loop(0, fl // tm, dw2, 0)
        send_g(1, b, False)
    for b in range(2):
        for h in range(2):
            def dw1(t, _):
                s = pl.ds(pl.multiple_of(t * tm, tm), tm)
                w1[b, pl.ds(pl.multiple_of(h * hd + t * tm, tm), tm), :] = dot_l(xs[h, :, s], g[b]).astype(BF)
                return 0

            lax.fori_loop(0, hd // tm, dw1, 0)
        send_g(0, b, False)

    loss_ref[...] = lbuf[2]

    for i in range(nl):
        rr = nl * c + i
        row = rr + odd * (ntp - 1 - 2 * rr)
        same = (row == y) & (lax.div(y, 2) == c)
        for n, (src, buf) in enumerate(((w1_hbm, w1), (w2_hbm, w2))):
            @pl.when(jnp.logical_not(same))
            def _():
                rcopy(src.at[i], buf.at[0], ws_sem.at[n, i], wr_sem.at[n, 0], mate).wait_send()

    def drain(m, _):
        cp_rs(zs, zr, m, fz_s, fz_r).wait_send()
        cp_ag(ds, c, m, ba_s, ba_r).wait_send()

        @pl.when(jnp.logical_not(last))
        def _():
            cp_link(hs, xs, m, fl_s, fl_r, nxt).wait_send()

        @pl.when(jnp.logical_not(first))
        def _():
            cp_ag(xs, c, m, fa_s, fa_r).wait_send()
            cp_rs(zsb, zrb, m, bz_s, bz_r).wait_send()
            cp_link(hb, ds, m, bl_s, bl_r, prv).wait_send()

        return 0

    lax.fori_loop(0, nc, drain, 0)

    @pl.when(jnp.logical_not(first))
    def _():
        rcopy(lbuf.at[2], lbuf.at[2], ls_sem.at[1], lr_sem.at[1], prv).wait_send()

    for n in range(2):
        buf, out = ((w1, g1_hbm), (w2, g2_hbm))[n]
        for b in range(2):
            send_g(n, b, True)
        for i in range(nl):
            rcopy(buf.at[0], out.at[i], gs_sem.at[n, 0], gr_sem.at[n, i], mate).wait_recv()


def solution(mesh):
    ntp = mesh.shape['tp']
    npp = mesh.shape['pp']

    def body(x, target, w1, w2):
        nm, b, d = x.shape
        _, nl, _, fl = w1.shape
        ntok = nm * b
        hd = d // 2
        nc = ntok // CHUNK
        dma = pltpu.SemaphoreType.DMA
        any_ = pl.BlockSpec(memory_space=pl.ANY)
        vm = pltpu.VMEM
        g1, g2, loss = pl.pallas_call(
            functools.partial(kernel, ntp, npp, (nm * b) ** -0.5),
            out_shape=(jax.ShapeDtypeStruct((nl, d, fl), BF), jax.ShapeDtypeStruct((nl, fl, d), BF),
                       jax.ShapeDtypeStruct((8, 128), F32)),
            in_specs=[any_] * 4,
            out_specs=(any_, any_, pl.BlockSpec(memory_space=pltpu.VMEM)),
            scratch_shapes=[
                vm((2, d, fl), BF), vm((2, fl, d), BF),
                vm((2, ntok, hd), BF), vm((2, ntok, hd), BF),
                vm((2, ntok, fl), BF), vm((2, ntok, fl), BF),
                vm((ntok, hd), BF), vm((ntok, hd), BF),
                vm((ntok, hd), BF), vm((ntok, hd), BF), vm((ntok, hd), BF), vm((ntok, hd), BF),
                vm((2, CHUNK, fl), BF), vm((CHUNK, hd), F32), vm((8, 128), F32), vm((3, 8, 128), F32),
                dma((3,)), dma((2, nl)), dma((2, 2)), dma((2, 2)), dma((2, nl)),
                dma((nc,)), dma((nc,)), dma((nc,)), dma((nc,)), dma((nc,)), dma((nc,)),
                dma((nc,)), dma((nc,)), dma((nc,)), dma((nc,)), dma((nc,)), dma((nc,)),
                dma((2,)), dma((2,)),
            ],
            compiler_params=pltpu.CompilerParams(collective_id=0, has_side_effects=True,
                                                 vmem_limit_bytes=62 * 2 ** 20),
            name='step',
        )(x.reshape(ntok, d), target.reshape(ntok, d), w1[0], w2[0])
        loss = jnp.sum(loss) * (0.5 / (nm * b * d))
        return g1.astype(F32)[None], g2.astype(F32)[None], loss.reshape(1)

    wspec1 = P(('dp', 'pp'), None, None, 'tp')
    wspec2 = P(('dp', 'pp'), None, 'tp', None)
    return jax.shard_map(body, mesh=mesh,
                         in_specs=(P('dp', None, None), P('dp', None, None), wspec1, wspec2),
                         out_specs=(wspec1, wspec2, P('dp')), check_vma=False)
```

```python
import functools
import math
import jax
import jax.numpy as jnp
from jax import lax
from jax.experimental import pallas as pl
from jax.experimental.pallas import tpu as pltpu
from jax.sharding import PartitionSpec as P

GC = math.sqrt(2.0 / math.pi)
BF = jnp.bfloat16
F32 = jnp.float32
MESH = pl.DeviceIdType.MESH
CHUNK = 128
PARTS = 4
VIA = 3


def gelu_parts(v):
    return jnp.tanh(GC * (v + 0.044715 * v * v * v))


def dot(a, b):
    return jnp.dot(a, b, preferred_element_type=F32)


def dot_l(a, b):
    return lax.dot_general(a, b, (((0,), (0,)), ((), ())), preferred_element_type=F32)


def kernel(ntp, npp, scale, x_hbm, t_hbm, w1_hbm, w2_hbm, g1_hbm, g2_hbm, loss_ref,
           w1, w2, w1t, w2t, xs, ds, u, g, hs, hb, zs, zr, zsb, zrb, a_buf, zown, lacc, lbuf, rw1, rw2, rg1, rg2,
           in_sem, ws_sem, wr_sem, gs_sem, gr_sem, rws, rwr, rgs, rgr, fl_s, fl_r, fa_s, fa_r, fz_s, fz_r,
           bl_s, bl_r, ba_s, ba_r, bz_s, bz_r, ls_sem, lr_sem):
    ntok, hd = hs.shape
    nl, d, fl = w1_hbm.shape
    ct = CHUNK
    nc = ntok // ct
    y = lax.axis_index('tp')
    pp = lax.axis_index('pp')
    c = lax.rem(pp, 2)
    o = 1 - c
    xc = lax.div(pp, 2)
    odd = lax.rem(xc, 2)
    r = y + odd * (ntp - 1 - 2 * y)
    k = xc * ntp + r
    nk = ntp * npp // 2
    first = k == 0
    last = k == nk - 1
    step = 1 - 2 * odd
    fwd_end = jnp.where(r == ntp - 1, 1, 0)
    bwd_end = jnp.where(r == 0, 1, 0)
    nxt = {'tp': y + step * (1 - fwd_end), 'pp': jnp.where(last, c, pp + 2 * fwd_end)}
    nxt['tp'] = jnp.where(last, 0, nxt['tp'])
    prv = {'tp': y - step * (1 - bwd_end), 'pp': jnp.where(first, npp - 2 + c, pp - 2 * bwd_end)}
    row_end = (ntp - 1) * (1 - lax.rem(npp // 2 - 1, 2))
    prv['tp'] = jnp.where(first, row_end, prv['tp'])
    mate = {'tp': y, 'pp': 2 * xc + o}

    barrier = pltpu.get_barrier_semaphore()
    for j in range(1, 2 * ntp):
        idx = lax.rem(y * 2 + c + j, 2 * ntp)
        pl.semaphore_signal(barrier, inc=1, device_id={'tp': lax.div(idx, 2), 'pp': 2 * xc + lax.rem(idx, 2)},
                            device_id_type=MESH)
    pl.semaphore_signal(barrier, inc=1, device_id=nxt, device_id_type=MESH)
    pl.semaphore_signal(barrier, inc=1, device_id=prv, device_id_type=MESH)
    ncol = npp // 2
    src_col = xc == 0
    rel_col = xc == ncol - 1
    edge = src_col | rel_col
    other_col = ncol - 1 - xc

    @pl.when(edge)
    def _():
        for j in range(2 * ntp):
            pl.semaphore_signal(barrier, inc=1, device_id={'tp': j // 2, 'pp': 2 * other_col + j % 2},
                                device_id_type=MESH)

    pl.semaphore_wait(barrier, 2 * ntp + 1 + jnp.where(edge, 2 * ntp, 0))

    def rcopy(src, dst, ss, rs, dev):
        return pltpu.make_async_remote_copy(src_ref=src, dst_ref=dst, send_sem=ss, recv_sem=rs,
                                            device_id=dev, device_id_type=MESH)

    rp = d // PARTS
    parts = [pl.ds(p * rp, rp) for p in range(PARTS)]
    wsrc = (w1_hbm, w2_hbm)
    wbuf = (w1, w2)
    rwb = (rw1, rw2)
    rgb = (rg1, rg2)
    gout = (g1_hbm, g2_hbm)
    cq = lax.div(y, 2)
    bq = lax.rem(y, 2)
    far = lax.rem(y + ntp // 2, ntp)
    kd = PARTS - VIA

    def w_copy(i, n, p):
        rr = nl * c + i
        row = rr + odd * (ntp - 1 - 2 * rr)
        src, dst = wsrc[n].at[i, parts[p]], wbuf[n].at[bq, parts[p]]
        ss, rs = ws_sem.at[n, i, p], wr_sem.at[n, bq, p]
        same = (row == y) & (cq == c)
        direct = functools.partial(rcopy, src, dst, ss, rs, {'tp': row, 'pp': 2 * xc + cq})
        relay = functools.partial(rcopy, src, rwb[n].at[max(p - kd, 0)], ss, rwr.at[n, max(p - kd, 0)],
                                  {'tp': row, 'pp': 2 * (ncol - 1) + cq})
        local = functools.partial(pltpu.make_async_copy, src, dst, rs)
        return same, src_col & (row == far), direct, relay, local

    def send(same, via, direct, relay, local, p):
        @pl.when(same)
        def _():
            local().start()

        if p < kd:
            @pl.when(jnp.logical_not(same))
            def _():
                direct().start()
        else:
            @pl.when(jnp.logical_not(same) & jnp.logical_not(via))
            def _():
                direct().start()

            @pl.when(via)
            def _():
                relay().start()

    def send_w():
        for n in range(2):
            for p in reversed(range(PARTS)):
                for i in range(nl):
                    send(*w_copy(i, n, p), p)

    home = {'tp': y, 'pp': c}
    far_b = lax.rem(far, 2)
    far_i = lax.rem(far, nl)

    def relay_w():
        for wait in (False, True):
            for n in range(2):
                for p in reversed(range(kd, PARTS)):
                    slot = rwb[n].at[p - kd]
                    fwd_cp = rcopy(slot, wbuf[n].at[far_b, parts[p]], rws.at[n, p - kd], wr_sem.at[n, far_b, p], home)
                    if wait:
                        fwd_cp.wait_send()
                    else:
                        rcopy(slot, slot, rws.at[n, p - kd], rwr.at[n, p - kd], home).wait_recv()
                        fwd_cp.start()

    pl.when(rel_col & (lax.div(far, 2) == c))(relay_w)
    send_w()

    @pl.when(first)
    def _():
        for h in range(2):
            pltpu.make_async_copy(x_hbm.at[:, pl.ds(h * hd, hd)], xs.at[h], in_sem.at[h]).start()

    @pl.when(last)
    def _():
        pltpu.make_async_copy(t_hbm.at[:, pl.ds(pl.multiple_of(c * hd, hd), hd)], hs, in_sem.at[2]).start()

    lacc[...] = jnp.zeros_like(lacc)

    for n in range(2):
        for b in range(2):
            for p in range(PARTS):
                rcopy(wsrc[n].at[0, parts[p]], wbuf[n].at[b, parts[p]], ws_sem.at[n, 0, p], wr_sem.at[n, b, p],
                      mate).wait_recv()

    @pl.when(first)
    def _():
        for h in range(2):
            pltpu.make_async_copy(x_hbm.at[:, pl.ds(h * hd, hd)], xs.at[h], in_sem.at[h]).wait()

    @pl.when(last)
    def _():
        pltpu.make_async_copy(t_hbm.at[:, pl.ds(pl.multiple_of(c * hd, hd), hd)], hs, in_sem.at[2]).wait()

    def rows(m):
        return pl.ds(pl.multiple_of(m * ct, ct), ct)

    def cp_link(buf, store, m, ss, rs, dev):
        return rcopy(buf.at[rows(m)], store.at[c, rows(m)], ss.at[m], rs.at[m], dev)

    def cp_ag(store, half, m, ss, rs):
        return rcopy(store.at[half, rows(m)], store.at[half, rows(m)], ss.at[m], rs.at[m], mate)

    def cp_rs(src, dst, m, ss, rs):
        return rcopy(src.at[rows(m)], dst.at[rows(m)], ss.at[m], rs.at[m], mate)

    def get_f(m):
        cp_link(hs, xs, m, fl_s, fl_r, nxt).wait_recv()
        cp_ag(xs, c, m, fa_s, fa_r).start()

    @pl.when(jnp.logical_not(first))
    def _():
        get_f(0)

    half_o = pl.ds(pl.multiple_of(o * hd, hd), hd)
    half_c = pl.ds(pl.multiple_of(c * hd, hd), hd)
    tn = fl // 2

    def fwd(m, _):
        @pl.when(jnp.logical_not(first))
        def _():
            cp_ag(xs, o, m, fa_s, fa_r).wait_recv()

        rw = rows(m)
        for q in range(2):
            for t in range(fl // tn):
                s = pl.ds(t * tn, tn)
                v = (dot(xs[0, rw, :], w1[q, :hd, s]) + dot(xs[1, rw, :], w1[q, hd:, s])).astype(BF)
                u[q, rw, s] = v
                v = v.astype(F32)
                a_buf[q, :, s] = (0.5 * v * (1.0 + gelu_parts(v))).astype(BF)
        zs[rw, :] = (dot(a_buf[0], w2[0, :, half_o]) + dot(a_buf[1], w2[1, :, half_o])).astype(BF)
        cp_rs(zs, zr, m, fz_s, fz_r).start()
        zown[...] = (xs[c, rw, :].astype(F32)
                     + (dot(a_buf[0], w2[0, :, half_c]) + dot(a_buf[1], w2[1, :, half_c])))

        @pl.when(jnp.logical_not(first) & (m + 1 < nc))
        def _():
            get_f(m + 1)

        cp_rs(zs, zr, m, fz_s, fz_r).wait_recv()
        out = (zown[...] + zr[rw, :].astype(F32)).astype(BF)

        @pl.when(jnp.logical_not(last))
        def _():
            hs[rw, :] = out
            cp_link(hs, xs, m, fl_s, fl_r, nxt).start()

        @pl.when(last)
        def _():
            diff = out.astype(F32) - hs[rw, :].astype(F32)
            ds[c, rw, :] = (diff * scale).astype(BF)
            sq = jnp.sum((diff * diff).reshape(ct // 8, 8, hd), axis=0)
            tot = lacc[...]
            for j in range(hd // 128):
                tot = tot + sq[:, j * 128:(j + 1) * 128]
            lacc[...] = tot

        return 0

    def transpose_w():
        tt = 256
        for b in range(2):
            def t1(t, _):
                s = pl.ds(pl.multiple_of(t * tt, tt), tt)
                w1t[b, :, s] = w1[b, s, :].T
                return 0

            def t2(t, _):
                s = pl.ds(pl.multiple_of(t * tt, tt), tt)
                w2t[b, :, s] = w2[b, s, :].T
                return 0

            lax.fori_loop(0, d // tt, t1, 0)
            lax.fori_loop(0, fl // tt, t2, 0)

    early = k >= nk // 2
    pl.when(early)(transpose_w)
    lax.fori_loop(0, nc, fwd, 0)
    pl.when(jnp.logical_not(early))(transpose_w)

    def get_b(m):
        @pl.when(jnp.logical_not(last))
        def _():
            cp_link(hb, ds, m, bl_s, bl_r, prv).wait_recv()

        cp_ag(ds, c, m, ba_s, ba_r).start()

    get_b(0)

    def bwd(m, _):
        cp_ag(ds, o, m, ba_s, ba_r).wait_recv()
        rw = rows(m)
        for q in range(2):
            for t in range(fl // tn):
                s = pl.ds(t * tn, tn)
                da = dot(ds[0, rw, :], w2t[q, :hd, s]) + dot(ds[1, rw, :], w2t[q, hd:, s])
                v = u[q, rw, s].astype(F32)
                th = gelu_parts(v)
                gp = 0.5 * (1.0 + th) + 0.5 * v * (1.0 - th * th) * GC * (1.0 + 0.134145 * v * v)
                g[q, rw, s] = (gp * da).astype(BF)
                u[q, rw, s] = (0.5 * v * (1.0 + th)).astype(BF)

        @pl.when(jnp.logical_not(first))
        def _():
            zsb[rw, :] = (dot(g[0, rw, :], w1t[0, :, half_o]) + dot(g[1, rw, :], w1t[1, :, half_o])).astype(BF)
            cp_rs(zsb, zrb, m, bz_s, bz_r).start()
            zown[...] = (ds[c, rw, :].astype(F32)
                         + (dot(g[0, rw, :], w1t[0, :, half_c]) + dot(g[1, rw, :], w1t[1, :, half_c])))

        @pl.when(m + 1 < nc)
        def _():
            get_b(m + 1)

        @pl.when(jnp.logical_not(first))
        def _():
            cp_rs(zsb, zrb, m, bz_s, bz_r).wait_recv()
            hb[rw, :] = (zown[...] + zrb[rw, :].astype(F32)).astype(BF)
            cp_link(hb, ds, m, bl_s, bl_r, prv).start()

        return 0

    lax.fori_loop(0, nc, bwd, 0)

    @pl.when(last)
    def _():
        lbuf[0] = lacc[...]
        cp = rcopy(lbuf.at[0], lbuf.at[1], ls_sem.at[0], lr_sem.at[0], mate)
        cp.start()
        cp.wait()
        lbuf[2] = lbuf[0] + lbuf[1]

    @pl.when(jnp.logical_not(last))
    def _():
        rcopy(lbuf.at[2], lbuf.at[2], ls_sem.at[1], lr_sem.at[1], prv).wait_recv()

    @pl.when(jnp.logical_not(first))
    def _():
        rcopy(lbuf.at[2], lbuf.at[2], ls_sem.at[1], lr_sem.at[1], prv).start()

    i_own = lax.rem(r, nl)
    src_core = lax.div(r, nl)

    def g_copy(n, b, p):
        row = 2 * c + b
        src, dst = wbuf[n].at[b, parts[p]], gout[n].at[i_own, parts[p]]
        ss, rs = gs_sem.at[n, b, p], gr_sem.at[n, i_own, p]
        same = (row == y) & (src_core == c)
        direct = functools.partial(rcopy, src, dst, ss, rs, {'tp': row, 'pp': 2 * xc + src_core})
        relay = functools.partial(rcopy, src, rgb[n].at[max(p - kd, 0)], ss, rgr.at[n, max(p - kd, 0)],
                                  {'tp': row, 'pp': 2 * (ncol - 1) + src_core})
        local = functools.partial(pltpu.make_async_copy, src, dst, rs)
        return same, src_col & (row == far), direct, relay, local

    def send_g(n, b):
        for p in reversed(range(PARTS)):
            send(*g_copy(n, b, p), p)

    def relay_g():
        for wait in (False, True):
            for n in (1, 0):
                for p in reversed(range(kd, PARTS)):
                    slot = rgb[n].at[p - kd]
                    fwd_cp = rcopy(slot, gout[n].at[far_i, parts[p]], rgs.at[n, p - kd], gr_sem.at[n, far_i, p], home)
                    if wait:
                        fwd_cp.wait_send()
                    else:
                        rcopy(slot, slot, rgs.at[n, p - kd], rgr.at[n, p - kd], home).wait_recv()
                        fwd_cp.start()

    tm = 256

    for b in range(2):
        def dw2(t, _):
            s = pl.ds(pl.multiple_of(t * tm, tm), tm)
            for h in range(2):
                w2[b, s, h * hd:(h + 1) * hd] = dot_l(u[b, :, s], ds[h]).astype(BF)
            return 0

        lax.fori_loop(0, fl // tm, dw2, 0)
        send_g(1, b)
    for b in range(2):
        for h in range(2):
            def dw1(t, _):
                s = pl.ds(pl.multiple_of(t * tm, tm), tm)
                w1[b, pl.ds(pl.multiple_of(h * hd + t * tm, tm), tm), :] = dot_l(xs[h, :, s], g[b]).astype(BF)
                return 0

            lax.fori_loop(0, hd // tm, dw1, 0)
        send_g(0, b)

    loss_ref[...] = lbuf[2]
    pl.when(rel_col & (lax.div(far, nl) == c))(relay_g)

    for i in range(nl):
        for n in range(2):
            for p in range(PARTS):
                same, _, direct, _, _ = w_copy(i, n, p)

                @pl.when(jnp.logical_not(same))
                def _():
                    direct().wait_send()

    def drain(m, _):
        cp_rs(zs, zr, m, fz_s, fz_r).wait_send()
        cp_ag(ds, c, m, ba_s, ba_r).wait_send()

        @pl.when(jnp.logical_not(last))
        def _():
            cp_link(hs, xs, m, fl_s, fl_r, nxt).wait_send()

        @pl.when(jnp.logical_not(first))
        def _():
            cp_ag(xs, c, m, fa_s, fa_r).wait_send()
            cp_rs(zsb, zrb, m, bz_s, bz_r).wait_send()
            cp_link(hb, ds, m, bl_s, bl_r, prv).wait_send()

        return 0

    lax.fori_loop(0, nc, drain, 0)

    @pl.when(jnp.logical_not(first))
    def _():
        rcopy(lbuf.at[2], lbuf.at[2], ls_sem.at[1], lr_sem.at[1], prv).wait_send()

    for n in range(2):
        for p in range(PARTS):
            for b in range(2):
                same, _, direct, _, _ = g_copy(n, b, p)

                @pl.when(jnp.logical_not(same))
                def _():
                    direct().wait_send()

            for i in range(nl):
                rcopy(wbuf[n].at[0, parts[p]], gout[n].at[i, parts[p]], gs_sem.at[n, 0, p], gr_sem.at[n, i, p],
                      mate).wait_recv()


def solution(mesh):
    ntp = mesh.shape['tp']
    npp = mesh.shape['pp']

    def body(x, target, w1, w2):
        nm, b, d = x.shape
        _, nl, _, fl = w1.shape
        ntok = nm * b
        hd = d // 2
        nc = ntok // CHUNK
        dma = pltpu.SemaphoreType.DMA
        any_ = pl.BlockSpec(memory_space=pl.ANY)
        vm = pltpu.VMEM
        g1, g2, loss = pl.pallas_call(
            functools.partial(kernel, ntp, npp, (nm * b) ** -0.5),
            out_shape=(jax.ShapeDtypeStruct((nl, d, fl), BF), jax.ShapeDtypeStruct((nl, fl, d), BF),
                       jax.ShapeDtypeStruct((8, 128), F32)),
            in_specs=[any_] * 4,
            out_specs=(any_, any_, pl.BlockSpec(memory_space=pltpu.VMEM)),
            scratch_shapes=[
                vm((2, d, fl), BF), vm((2, fl, d), BF), vm((2, fl, d), BF), vm((2, d, fl), BF),
                vm((2, ntok, hd), BF), vm((2, ntok, hd), BF),
                vm((2, ntok, fl), BF), vm((2, ntok, fl), BF),
                vm((ntok, hd), BF), vm((ntok, hd), BF),
                vm((ntok, hd), BF), vm((ntok, hd), BF), vm((ntok, hd), BF), vm((ntok, hd), BF),
                vm((2, CHUNK, fl), BF), vm((CHUNK, hd), F32), vm((8, 128), F32), vm((3, 8, 128), F32),
                vm((VIA, d // PARTS, fl), BF), vm((VIA, fl // PARTS, d), BF),
                vm((VIA, d // PARTS, fl), BF), vm((VIA, fl // PARTS, d), BF),
                dma((3,)), dma((2, nl, PARTS)), dma((2, 2, PARTS)), dma((2, 2, PARTS)), dma((2, nl, PARTS)),
                dma((2, VIA)), dma((2, VIA)), dma((2, VIA)), dma((2, VIA)),
                dma((nc,)), dma((nc,)), dma((nc,)), dma((nc,)), dma((nc,)), dma((nc,)),
                dma((nc,)), dma((nc,)), dma((nc,)), dma((nc,)), dma((nc,)), dma((nc,)),
                dma((2,)), dma((2,)),
            ],
            compiler_params=pltpu.CompilerParams(collective_id=0, has_side_effects=True,
                                                 vmem_limit_bytes=62 * 2 ** 20),
            name='step',
        )(x.reshape(ntok, d), target.reshape(ntok, d), w1[0], w2[0])
        loss = jnp.sum(loss) * (0.5 / (nm * b * d))
        return g1.astype(F32)[None], g2.astype(F32)[None], loss.reshape(1)

    wspec1 = P(('dp', 'pp'), None, None, 'tp')
    wspec2 = P(('dp', 'pp'), None, 'tp', None)
    return jax.shard_map(body, mesh=mesh,
                         in_specs=(P('dp', None, None), P('dp', None, None), wspec1, wspec2),
                         out_specs=(wspec1, wspec2, P('dp')), check_vma=False)
```

```python
import functools
import math
import jax
import jax.numpy as jnp
from jax import lax
from jax.experimental import pallas as pl
from jax.experimental.pallas import tpu as pltpu
from jax.sharding import PartitionSpec as P

GC = math.sqrt(2.0 / math.pi)
BF = jnp.bfloat16
F32 = jnp.float32
MESH = pl.DeviceIdType.MESH
CHUNK = 128
PARTS = 4
VIA = 4


def gelu_parts(v):
    return jnp.tanh(GC * (v + 0.044715 * v * v * v))


def dot(a, b):
    return jnp.dot(a, b, preferred_element_type=F32)


def dot_l(a, b):
    return lax.dot_general(a, b, (((0,), (0,)), ((), ())), preferred_element_type=F32)


def kernel(ntp, npp, scale, x_hbm, t_hbm, w1_hbm, w2_hbm, g1_hbm, g2_hbm, loss_ref,
           w1, w2, w1t, w2t, part, xs, ds, u, g, hs, hb, zs, zr, zsb, zrb, a_buf, zown, lacc, lbuf, rg1, rg2,
           in_sem, ws_sem, wr_sem, gs_sem, gr_sem, rws, rwr, rgs, rgr, fl_s, fl_r, fa_s, fa_r, fz_s, fz_r,
           bl_s, bl_r, ba_s, ba_r, bz_s, bz_r, ls_sem, lr_sem):
    ntok, hd = hs.shape
    nl, d, fl = w1_hbm.shape
    ct = CHUNK
    nc = ntok // ct
    y = lax.axis_index('tp')
    pp = lax.axis_index('pp')
    c = lax.rem(pp, 2)
    o = 1 - c
    xc = lax.div(pp, 2)
    odd = lax.rem(xc, 2)
    r = y + odd * (ntp - 1 - 2 * y)
    k = xc * ntp + r
    nk = ntp * npp // 2
    first = k == 0
    last = k == nk - 1
    step = 1 - 2 * odd
    fwd_end = jnp.where(r == ntp - 1, 1, 0)
    bwd_end = jnp.where(r == 0, 1, 0)
    nxt = {'tp': y + step * (1 - fwd_end), 'pp': jnp.where(last, c, pp + 2 * fwd_end)}
    nxt['tp'] = jnp.where(last, 0, nxt['tp'])
    prv = {'tp': y - step * (1 - bwd_end), 'pp': jnp.where(first, npp - 2 + c, pp - 2 * bwd_end)}
    row_end = (ntp - 1) * (1 - lax.rem(npp // 2 - 1, 2))
    prv['tp'] = jnp.where(first, row_end, prv['tp'])
    mate = {'tp': y, 'pp': 2 * xc + o}

    barrier = pltpu.get_barrier_semaphore()
    for j in range(1, 2 * ntp):
        idx = lax.rem(y * 2 + c + j, 2 * ntp)
        pl.semaphore_signal(barrier, inc=1, device_id={'tp': lax.div(idx, 2), 'pp': 2 * xc + lax.rem(idx, 2)},
                            device_id_type=MESH)
    pl.semaphore_signal(barrier, inc=1, device_id=nxt, device_id_type=MESH)
    pl.semaphore_signal(barrier, inc=1, device_id=prv, device_id_type=MESH)
    ncol = npp // 2
    src_col = xc == 0
    rel_col = xc == ncol - 1
    edge = src_col | rel_col
    other_col = ncol - 1 - xc

    @pl.when(edge)
    def _():
        for j in range(2 * ntp):
            pl.semaphore_signal(barrier, inc=1, device_id={'tp': j // 2, 'pp': 2 * other_col + j % 2},
                                device_id_type=MESH)

    pl.semaphore_wait(barrier, 2 * ntp + 1 + jnp.where(edge, 2 * ntp, 0))

    def rcopy(src, dst, ss, rs, dev):
        return pltpu.make_async_remote_copy(src_ref=src, dst_ref=dst, send_sem=ss, recv_sem=rs,
                                            device_id=dev, device_id_type=MESH)

    rp = d // PARTS
    parts = [pl.ds(p * rp, rp) for p in range(PARTS)]
    wsrc = (w1_hbm, w2_hbm)
    wbuf = (w1, w2)
    rgb = (rg1, rg2)
    gout = (g1_hbm, g2_hbm)
    cq = lax.div(y, 2)
    bq = lax.rem(y, 2)
    far = lax.rem(y + ntp // 2, ntp)
    kd = PARTS - VIA

    def w_copy(i, n, p):
        rr = nl * c + i
        row = rr + odd * (ntp - 1 - 2 * rr)
        src, dst = wsrc[n].at[i, parts[p]], wbuf[n].at[bq, parts[p]]
        ss, rs = ws_sem.at[n, i, p], wr_sem.at[n, bq, p]
        same = (row == y) & (cq == c)
        direct = functools.partial(rcopy, src, dst, ss, rs, {'tp': row, 'pp': 2 * xc + cq})
        relay = functools.partial(rcopy, src, g.at[n, parts[max(p - kd, 0)]], ss, rwr.at[n, max(p - kd, 0)],
                                  {'tp': row, 'pp': 2 * (ncol - 1) + cq})
        local = functools.partial(pltpu.make_async_copy, src, dst, rs)
        return same, src_col & (row == far), direct, relay, local

    def send(same, via, direct, relay, local, p):
        @pl.when(same)
        def _():
            local().start()

        if p < kd:
            @pl.when(jnp.logical_not(same))
            def _():
                direct().start()
        else:
            @pl.when(jnp.logical_not(same) & jnp.logical_not(via))
            def _():
                direct().start()

            @pl.when(via)
            def _():
                relay().start()

    def send_w():
        for n in range(2):
            for p in reversed(range(PARTS)):
                for i in range(nl):
                    send(*w_copy(i, n, p), p)

    home = {'tp': y, 'pp': c}
    far_b = lax.rem(far, 2)
    far_i = lax.rem(far, nl)

    def relay_w():
        for wait in (False, True):
            for n in range(2):
                for p in reversed(range(kd, PARTS)):
                    slot = g.at[n, parts[p - kd]]
                    fwd_cp = rcopy(slot, wbuf[n].at[far_b, parts[p]], rws.at[n, p - kd], wr_sem.at[n, far_b, p], home)
                    if wait:
                        fwd_cp.wait_send()
                    else:
                        rcopy(slot, slot, rws.at[n, p - kd], rwr.at[n, p - kd], home).wait_recv()
                        fwd_cp.start()

    pl.when(rel_col & (lax.div(far, 2) == c))(relay_w)
    send_w()

    @pl.when(first)
    def _():
        for h in range(2):
            pltpu.make_async_copy(x_hbm.at[:, pl.ds(h * hd, hd)], xs.at[h], in_sem.at[h]).start()

    @pl.when(last)
    def _():
        pltpu.make_async_copy(t_hbm.at[:, pl.ds(pl.multiple_of(c * hd, hd), hd)], hs, in_sem.at[2]).start()

    lacc[...] = jnp.zeros_like(lacc)

    for n in range(2):
        for b in range(2):
            for p in range(PARTS):
                rcopy(wsrc[n].at[0, parts[p]], wbuf[n].at[b, parts[p]], ws_sem.at[n, 0, p], wr_sem.at[n, b, p],
                      mate).wait_recv()

    @pl.when(first)
    def _():
        for h in range(2):
            pltpu.make_async_copy(x_hbm.at[:, pl.ds(h * hd, hd)], xs.at[h], in_sem.at[h]).wait()

    @pl.when(last)
    def _():
        pltpu.make_async_copy(t_hbm.at[:, pl.ds(pl.multiple_of(c * hd, hd), hd)], hs, in_sem.at[2]).wait()

    def rows(m):
        return pl.ds(pl.multiple_of(m * ct, ct), ct)

    def cp_link(buf, store, m, ss, rs, dev):
        return rcopy(buf.at[rows(m)], store.at[c, rows(m)], ss.at[m], rs.at[m], dev)

    def cp_ag(store, half, m, ss, rs):
        return rcopy(store.at[half, rows(m)], store.at[half, rows(m)], ss.at[m], rs.at[m], mate)

    def cp_rs(src, dst, m, ss, rs):
        return rcopy(src.at[rows(m)], dst.at[rows(m)], ss.at[m], rs.at[m], mate)

    def get_f(m):
        cp_link(hs, xs, m, fl_s, fl_r, nxt).wait_recv()
        cp_ag(xs, c, m, fa_s, fa_r).start()

    @pl.when(jnp.logical_not(first))
    def _():
        get_f(0)

    half_o = pl.ds(pl.multiple_of(o * hd, hd), hd)
    half_c = pl.ds(pl.multiple_of(c * hd, hd), hd)
    tn = fl // 2

    def fwd(m, _):
        rw = rows(m)
        mine = xs[c, rw, :]
        for q in range(2):
            part[q] = dot(mine, w1[q, half_c, :])

        @pl.when(jnp.logical_not(first))
        def _():
            cp_ag(xs, o, m, fa_s, fa_r).wait_recv()

        for q in range(2):
            for t in range(fl // tn):
                s = pl.ds(t * tn, tn)
                v = (part[q, :, s] + dot(xs[o, rw, :], w1[q, half_o, s])).astype(BF)
                u[q, rw, s] = v
                v = v.astype(F32)
                a_buf[q, :, s] = (0.5 * v * (1.0 + gelu_parts(v))).astype(BF)
        zs[rw, :] = (dot(a_buf[0], w2[0, :, half_o]) + dot(a_buf[1], w2[1, :, half_o])).astype(BF)
        cp_rs(zs, zr, m, fz_s, fz_r).start()
        zown[...] = (xs[c, rw, :].astype(F32)
                     + (dot(a_buf[0], w2[0, :, half_c]) + dot(a_buf[1], w2[1, :, half_c])))

        @pl.when(jnp.logical_not(first) & (m + 1 < nc))
        def _():
            get_f(m + 1)

        cp_rs(zs, zr, m, fz_s, fz_r).wait_recv()
        out = (zown[...] + zr[rw, :].astype(F32)).astype(BF)

        @pl.when(jnp.logical_not(last))
        def _():
            hs[rw, :] = out
            cp_link(hs, xs, m, fl_s, fl_r, nxt).start()

        @pl.when(last)
        def _():
            diff = out.astype(F32) - hs[rw, :].astype(F32)
            ds[c, rw, :] = (diff * scale).astype(BF)
            sq = jnp.sum((diff * diff).reshape(ct // 8, 8, hd), axis=0)
            tot = lacc[...]
            for j in range(hd // 128):
                tot = tot + sq[:, j * 128:(j + 1) * 128]
            lacc[...] = tot

        return 0

    def transpose_w():
        tt = 256
        for b in range(2):
            def t1(t, _):
                s = pl.ds(pl.multiple_of(t * tt, tt), tt)
                w1t[b, :, s] = w1[b, s, :].T
                return 0

            def t2(t, _):
                s = pl.ds(pl.multiple_of(t * tt, tt), tt)
                w2t[b, :, s] = w2[b, s, :].T
                return 0

            lax.fori_loop(0, d // tt, t1, 0)
            lax.fori_loop(0, fl // tt, t2, 0)

    early = k >= nk // 2
    pl.when(early)(transpose_w)
    lax.fori_loop(0, nc, fwd, 0)
    pl.when(jnp.logical_not(early))(transpose_w)

    def get_b(m):
        @pl.when(jnp.logical_not(last))
        def _():
            cp_link(hb, ds, m, bl_s, bl_r, prv).wait_recv()

        cp_ag(ds, c, m, ba_s, ba_r).start()

    get_b(0)

    def bwd(m, _):
        rw = rows(m)
        mine = ds[c, rw, :]
        for q in range(2):
            part[q] = dot(mine, w2t[q, half_c, :])
        cp_ag(ds, o, m, ba_s, ba_r).wait_recv()
        for q in range(2):
            for t in range(fl // tn):
                s = pl.ds(t * tn, tn)
                da = part[q, :, s] + dot(ds[o, rw, :], w2t[q, half_o, s])
                v = u[q, rw, s].astype(F32)
                th = gelu_parts(v)
                gp = 0.5 * (1.0 + th) + 0.5 * v * (1.0 - th * th) * GC * (1.0 + 0.134145 * v * v)
                g[q, rw, s] = (gp * da).astype(BF)
                u[q, rw, s] = (0.5 * v * (1.0 + th)).astype(BF)

        @pl.when(jnp.logical_not(first))
        def _():
            zsb[rw, :] = (dot(g[0, rw, :], w1t[0, :, half_o]) + dot(g[1, rw, :], w1t[1, :, half_o])).astype(BF)
            cp_rs(zsb, zrb, m, bz_s, bz_r).start()
            zown[...] = (ds[c, rw, :].astype(F32)
                         + (dot(g[0, rw, :], w1t[0, :, half_c]) + dot(g[1, rw, :], w1t[1, :, half_c])))

        @pl.when(m + 1 < nc)
        def _():
            get_b(m + 1)

        @pl.when(jnp.logical_not(first))
        def _():
            cp_rs(zsb, zrb, m, bz_s, bz_r).wait_recv()
            hb[rw, :] = (zown[...] + zrb[rw, :].astype(F32)).astype(BF)
            cp_link(hb, ds, m, bl_s, bl_r, prv).start()

        return 0

    lax.fori_loop(0, nc, bwd, 0)

    @pl.when(last)
    def _():
        lbuf[0] = lacc[...]
        cp = rcopy(lbuf.at[0], lbuf.at[1], ls_sem.at[0], lr_sem.at[0], mate)
        cp.start()
        cp.wait()
        lbuf[2] = lbuf[0] + lbuf[1]

    @pl.when(jnp.logical_not(last))
    def _():
        rcopy(lbuf.at[2], lbuf.at[2], ls_sem.at[1], lr_sem.at[1], prv).wait_recv()

    @pl.when(jnp.logical_not(first))
    def _():
        rcopy(lbuf.at[2], lbuf.at[2], ls_sem.at[1], lr_sem.at[1], prv).start()

    i_own = lax.rem(r, nl)
    src_core = lax.div(r, nl)

    def g_copy(n, b, p):
        row = 2 * c + b
        src, dst = wbuf[n].at[b, parts[p]], gout[n].at[i_own, parts[p]]
        ss, rs = gs_sem.at[n, b, p], gr_sem.at[n, i_own, p]
        same = (row == y) & (src_core == c)
        direct = functools.partial(rcopy, src, dst, ss, rs, {'tp': row, 'pp': 2 * xc + src_core})
        relay = functools.partial(rcopy, src, rgb[n].at[max(p - kd, 0)], ss, rgr.at[n, max(p - kd, 0)],
                                  {'tp': row, 'pp': 2 * (ncol - 1) + src_core})
        local = functools.partial(pltpu.make_async_copy, src, dst, rs)
        return same, src_col & (row == far), direct, relay, local

    def send_g(n, b):
        for p in reversed(range(PARTS)):
            send(*g_copy(n, b, p), p)

    def relay_g():
        for wait in (False, True):
            for n in (1, 0):
                for p in reversed(range(kd, PARTS)):
                    slot = rgb[n].at[p - kd]
                    fwd_cp = rcopy(slot, gout[n].at[far_i, parts[p]], rgs.at[n, p - kd], gr_sem.at[n, far_i, p], home)
                    if wait:
                        fwd_cp.wait_send()
                    else:
                        rcopy(slot, slot, rgs.at[n, p - kd], rgr.at[n, p - kd], home).wait_recv()
                        fwd_cp.start()

    tm = 256

    for b in range(2):
        def dw2(t, _):
            s = pl.ds(pl.multiple_of(t * tm, tm), tm)
            for h in range(2):
                w2[b, s, h * hd:(h + 1) * hd] = dot_l(u[b, :, s], ds[h]).astype(BF)
            return 0

        lax.fori_loop(0, fl // tm, dw2, 0)
        send_g(1, b)
    for b in range(2):
        for h in range(2):
            def dw1(t, _):
                s = pl.ds(pl.multiple_of(t * tm, tm), tm)
                w1[b, pl.ds(pl.multiple_of(h * hd + t * tm, tm), tm), :] = dot_l(xs[h, :, s], g[b]).astype(BF)
                return 0

            lax.fori_loop(0, hd // tm, dw1, 0)
        send_g(0, b)

    loss_ref[...] = lbuf[2]
    pl.when(rel_col & (lax.div(far, nl) == c))(relay_g)

    for i in range(nl):
        for n in range(2):
            for p in range(PARTS):
                same, _, direct, _, _ = w_copy(i, n, p)

                @pl.when(jnp.logical_not(same))
                def _():
                    direct().wait_send()

    def drain(m, _):
        cp_rs(zs, zr, m, fz_s, fz_r).wait_send()
        cp_ag(ds, c, m, ba_s, ba_r).wait_send()

        @pl.when(jnp.logical_not(last))
        def _():
            cp_link(hs, xs, m, fl_s, fl_r, nxt).wait_send()

        @pl.when(jnp.logical_not(first))
        def _():
            cp_ag(xs, c, m, fa_s, fa_r).wait_send()
            cp_rs(zsb, zrb, m, bz_s, bz_r).wait_send()
            cp_link(hb, ds, m, bl_s, bl_r, prv).wait_send()

        return 0

    lax.fori_loop(0, nc, drain, 0)

    @pl.when(jnp.logical_not(first))
    def _():
        rcopy(lbuf.at[2], lbuf.at[2], ls_sem.at[1], lr_sem.at[1], prv).wait_send()

    for n in range(2):
        for p in range(PARTS):
            for b in range(2):
                same, _, direct, _, _ = g_copy(n, b, p)

                @pl.when(jnp.logical_not(same))
                def _():
                    direct().wait_send()

            for i in range(nl):
                rcopy(wbuf[n].at[0, parts[p]], gout[n].at[i, parts[p]], gs_sem.at[n, 0, p], gr_sem.at[n, i, p],
                      mate).wait_recv()


def solution(mesh):
    ntp = mesh.shape['tp']
    npp = mesh.shape['pp']

    def body(x, target, w1, w2):
        nm, b, d = x.shape
        _, nl, _, fl = w1.shape
        ntok = nm * b
        hd = d // 2
        nc = ntok // CHUNK
        dma = pltpu.SemaphoreType.DMA
        any_ = pl.BlockSpec(memory_space=pl.ANY)
        vm = pltpu.VMEM
        g1, g2, loss = pl.pallas_call(
            functools.partial(kernel, ntp, npp, (nm * b) ** -0.5),
            out_shape=(jax.ShapeDtypeStruct((nl, d, fl), BF), jax.ShapeDtypeStruct((nl, fl, d), BF),
                       jax.ShapeDtypeStruct((8, 128), F32)),
            in_specs=[any_] * 4,
            out_specs=(any_, any_, pl.BlockSpec(memory_space=pltpu.VMEM)),
            scratch_shapes=[
                vm((2, d, fl), BF), vm((2, fl, d), BF), vm((2, fl, d), BF), vm((2, d, fl), BF),
                vm((2, CHUNK, fl), F32),
                vm((2, ntok, hd), BF), vm((2, ntok, hd), BF),
                vm((2, ntok, fl), BF), vm((2, ntok, fl), BF),
                vm((ntok, hd), BF), vm((ntok, hd), BF),
                vm((ntok, hd), BF), vm((ntok, hd), BF), vm((ntok, hd), BF), vm((ntok, hd), BF),
                vm((2, CHUNK, fl), BF), vm((CHUNK, hd), F32), vm((8, 128), F32), vm((3, 8, 128), F32),
                vm((VIA, d // PARTS, fl), BF), vm((VIA, fl // PARTS, d), BF),
                dma((3,)), dma((2, nl, PARTS)), dma((2, 2, PARTS)), dma((2, 2, PARTS)), dma((2, nl, PARTS)),
                dma((2, VIA)), dma((2, VIA)), dma((2, VIA)), dma((2, VIA)),
                dma((nc,)), dma((nc,)), dma((nc,)), dma((nc,)), dma((nc,)), dma((nc,)),
                dma((nc,)), dma((nc,)), dma((nc,)), dma((nc,)), dma((nc,)), dma((nc,)),
                dma((2,)), dma((2,)),
            ],
            compiler_params=pltpu.CompilerParams(collective_id=0, has_side_effects=True,
                                                 vmem_limit_bytes=62 * 2 ** 20),
            name='step',
        )(x.reshape(ntok, d), target.reshape(ntok, d), w1[0], w2[0])
        loss = jnp.sum(loss) * (0.5 / (nm * b * d))
        return g1.astype(F32)[None], g2.astype(F32)[None], loss.reshape(1)

    wspec1 = P(('dp', 'pp'), None, None, 'tp')
    wspec2 = P(('dp', 'pp'), None, 'tp', None)
    return jax.shard_map(body, mesh=mesh,
                         in_specs=(P('dp', None, None), P('dp', None, None), wspec1, wspec2),
                         out_specs=(wspec1, wspec2, P('dp')), check_vma=False)
```
